128 devices in a mesh: space: 32 (over x_lo, z, y), tm: 4 (over x_hi, core).
Axes of the slice: x: 4 (x_hi: 2, x_lo: 2; x = x_hi * 2 + x_lo), y: 4, z: 4, core: 2. Of those that a mesh axis runs over, the one named last changes fastest.
Arguments:
- innovations: bfloat16 [12, 32, 768, 1536], P('tm', None, 'space'), may hold values from -6 to 6
- obs_counts: int32 [12, 192, 384], P('tm', 'space'), may hold values from 0 to 3
- diffusion: float32 [32, 192, 384], P(None, 'space'), may hold values from 0.01 to 0.1
- courant: float32 [32, 192, 384], P(None, 'space'), may hold values from 0 to 0.4
Outputs:
- increment: float32 [32, 768, 1536], P('tm', 'space')
- residual: float32 [32, 192, 384], P('tm', 'space')
The draws below stay inside these ranges and needn't reach their ends.
All inputs are finite; a program needn't handle non-finite values.
Results may differ from the reference program's by a relative error of at most 0.0003.
Values sent between devices are 32-bit elements; how exact they have to be, the bound alone decides.
No kernel may reach another device: no remote copies, remote signals or barrier semaphores. Data moves between devices by JAX's collectives and lax.ppermute only.
A program may use at most 192 MiB of HBM per device.

```python
import math
import jax
import jax.numpy as jnp
from jax import lax

NLAT_F = 768
NLON_F = 1536
LEV = 32
ITERS = 3
NLAT = 192
NLON = 384
STEPS = 12


def touch_ends(entries, rng, smallest, high):
    spot = [jax.random.randint(jax.random.fold_in(rng, axis), (), 0, length) for axis, length in enumerate(entries.shape)]
    main_axis = entries.shape.index(max(entries.shape))
    next_to = spot[:main_axis] + [(spot[main_axis] + 1) % entries.shape[main_axis]] + spot[main_axis + 1:]
    return entries.at[tuple(spot)].set(smallest).at[tuple(next_to)].set(high)


def levels(rng, dims, split, smallest, high):
    factor_of, own = 1.0, jax.random.fold_in(rng, 6)
    for axis_at, parts in split:
        draws = jnp.exp(jax.random.uniform(jax.random.fold_in(own, axis_at), (parts,), jnp.float32, smallest / len(split), high / len(split)))
        factor_of = factor_of * jnp.repeat(draws, dims[axis_at] // parts).reshape([-1 if axis == axis_at else 1 for axis in range(len(dims))])
    return factor_of


def bell_draw(key, shape, spread, limit, cuts=(), held_as=jnp.bfloat16):
    entries = spread * jax.random.normal(key, shape, jnp.float32)
    if cuts:
        entries = entries * levels(key, shape, cuts, -0.22, 0.18)
    return jnp.clip(entries, -limit, limit).astype(held_as)


def setup_inputs(seed: int = 0) -> dict:
    key_list = jax.random.split(jax.random.key(seed), 5)
    innovations = bell_draw(key_list[0], (STEPS, LEV, NLAT_F, NLON_F), 1.0, 6.0, ((0, 4), (2, 32)))
    obs_counts = touch_ends(jax.random.randint(key_list[1], (STEPS, NLAT, NLON), 0, 4), jax.random.fold_in(key_list[1], 1), 0, 3).astype(jnp.int32)
    diffusion = jnp.clip(jnp.exp(math.log(0.1) - 2.3025851 * jax.random.uniform(key_list[2], (LEV, NLAT, NLON), jnp.float32) ** levels(key_list[2], (LEV, NLAT, NLON), ((1, 32),), -0.2, 0.2)), 0.01, 0.1)
    courant = jnp.clip(0.4 * jax.random.uniform(key_list[3], (LEV, NLAT, NLON), jnp.float32) ** levels(key_list[3], (LEV, NLAT, NLON), ((1, 32),), -0.2, 0.2), 0.0, 0.4)
    return {"innovations": innovations, "obs_counts": obs_counts, "diffusion": diffusion, "courant": courant}


def laplace(state_field):
    padded = jnp.pad(state_field, ((0, 0), (1, 1), (0, 0)))
    return padded[:, 2:, :] + padded[:, :-2, :] + jnp.roll(state_field, 1, 2) + jnp.roll(state_field, -1, 2) - 4.0 * state_field


def tangent(state_field, diffusion, courant):
    return state_field + diffusion * laplace(state_field) - courant * (state_field - jnp.roll(state_field, 1, 2))


def adjoint(state_field, diffusion, courant):
    carried = courant * state_field
    return state_field + laplace(diffusion * state_field) - carried + jnp.roll(carried, -1, 2)


def restrict(block_field):
    coarse = block_field.astype(jnp.float32).reshape(LEV, NLAT_F // 4, 4, NLON_F // 4, 4)
    return jnp.mean(coarse, axis=(2, 4))


def reference(innovations, obs_counts, diffusion, courant):
    weights = obs_counts.astype(jnp.float32)[:, None]
    forcing = weights * lax.map(restrict, innovations)

    def forward(state_field):
        records = []
        for step_no in range(STEPS):
            records.append(weights[step_no] * state_field)
            if step_no + 1 < STEPS:
                state_field = tangent(state_field, diffusion, courant)
        return jnp.stack(records)

    def backward(terms):
        current = terms[STEPS - 1]
        for step_no in range(STEPS - 2, -1, -1):
            current = terms[step_no] + adjoint(current, diffusion, courant)
        return current

    rhs_field = backward(forcing)
    control = jnp.zeros_like(rhs_field)
    residual = rhs_field
    direction = rhs_field
    norm_now = jnp.sum(residual * residual)
    for iter_no in range(ITERS):
        hessian_image = direction + backward(forward(direction))
        step_len = norm_now / jnp.sum(direction * hessian_image)
        control = control + step_len * direction
        residual = residual - step_len * hessian_image
        if iter_no + 1 < ITERS:
            norm_next = jnp.sum(residual * residual)
            direction = residual + (norm_next / norm_now) * direction
            norm_now = norm_next
    increment = jnp.repeat(jnp.repeat(control, 4, axis=1), 4, axis=2)
    return increment, residual
```

```python
import functools

import jax
import jax.numpy as jnp
import numpy as np
from jax import lax
from jax.experimental import pallas as pl
from jax.experimental.pallas import tpu as pltpu
from jax.sharding import Mesh
from jax.sharding import PartitionSpec as P

SPACE = ("space_0", "space_1", "space_2")
TM = ("tm_0", "tm_1")
SWAP = [(0, 1), (1, 0)]
F32 = jnp.float32
BF16 = jnp.bfloat16

NI, NJ = 24, 3
REGS = NI * NJ
ROWS = REGS * 8
STEPS = 12
ITERS = 3
VMEM = pl.BlockSpec(memory_space=pltpu.VMEM)
SMEM = pl.BlockSpec(memory_space=pltpu.SMEM)


def column_order():
    return (np.arange(128)[None, :] * NJ + np.arange(NJ)[:, None]).reshape(-1)


def matrices():
    order = column_order()
    pick = np.zeros((384, 384), np.float32)
    pick[order, np.arange(384)] = 1.0
    mean = np.repeat(pick, 4, axis=0) / 16.0
    spread = np.repeat(pick, 4, axis=0).T
    return (
        jnp.asarray(pick, BF16),
        jnp.asarray(mean, BF16),
        jnp.asarray(spread, BF16),
        jnp.asarray(pick.T, BF16),
    )


def exact_dot(x, one_hot):
    a = x.astype(BF16)
    rest = x - a.astype(F32)
    b = rest.astype(BF16)
    c = (rest - b.astype(F32)).astype(BF16)
    n = x.shape[0]
    y = jnp.dot(jnp.concatenate([a, b, c], 0), one_hot, preferred_element_type=F32)
    return y[:n] + y[n : 2 * n] + y[2 * n :]


def prepare_kernel(core_ref, counts_ref, diff_ref, cour_ref, pick_ref, out_ref, wt_ref, rows_ref):
    levels = diff_ref.shape[0]

    @pl.when(core_ref[0] == 0)
    def _():
        for k in range(levels):
            rows_ref[pl.ds(6 * k, 6), :] = diff_ref[k]

    @pl.when(core_ref[0] != 0)
    def _():
        for k in range(levels):
            rows_ref[pl.ds(6 * k, 6), :] = cour_ref[k]

    field = exact_dot(rows_ref[...], pick_ref[...])
    for k in range(levels):
        for j in range(NJ):
            out_ref[k, pl.ds(6 * j, 6), :] = field[6 * k : 6 * k + 6, 128 * j : 128 * j + 128]
    for t in range(3):
        w = jnp.dot(
            counts_ref[t].astype(F32).astype(BF16), pick_ref[...], preferred_element_type=F32
        )
        for k in range(8):
            wt_ref[t, pl.ds(6 * k, 6), :] = w
        for j in range(NJ):
            piece = w[:, 128 * j : 128 * j + 128]
            for k in range(levels):
                out_ref[k, pl.ds(18 + 18 * t + 6 * j, 6), :] = piece


def prepare(core, counts, diffusion, courant, pick):
    levels = diffusion.shape[0]
    return pl.pallas_call(
        prepare_kernel,
        name="prepare",
        out_shape=(
            jax.ShapeDtypeStruct((levels, 72, 128), F32),
            jax.ShapeDtypeStruct((3, 48, 384), F32),
        ),
        in_specs=[SMEM, VMEM, VMEM, VMEM, VMEM],
        out_specs=(VMEM, VMEM),
        scratch_shapes=[pltpu.VMEM((levels * 6, 384), F32)],
        cost_estimate=pl.CostEstimate(flops=10**9, bytes_accessed=3 * 10**6, transcendentals=0),
    )(core, counts, diffusion, courant, pick)


def restrict_kernel(fine_ref, wt_ref, mean_ref, out_ref, sums_ref):
    for t in range(3):
        sums = jnp.dot(fine_ref[t], mean_ref[...], preferred_element_type=F32)
        for j in range(NJ):
            sums_ref[3 * t + j] = sums[:, 128 * j : 128 * j + 128]
        for j in range(NJ):
            z = (
                sums_ref[3 * t + j, pl.ds(0, 48, stride=4), :]
                + sums_ref[3 * t + j, pl.ds(1, 48, stride=4), :]
                + sums_ref[3 * t + j, pl.ds(2, 48, stride=4), :]
                + sums_ref[3 * t + j, pl.ds(3, 48, stride=4), :]
            ) * wt_ref[t, :, 128 * j : 128 * j + 128]
            for k in range(8):
                out_ref[k, pl.ds(18 * t + 6 * j, 6), :] = z[6 * k : 6 * k + 6]


def restrict(fine, wt, mean):
    return pl.pallas_call(
        restrict_kernel,
        name="restrict",
        grid=(4,),
        out_shape=jax.ShapeDtypeStruct((32, 54, 128), F32),
        in_specs=[
            pl.BlockSpec((3, 192, 1536), lambda g: (0, g, 0)),
            pl.BlockSpec((3, 48, 384), lambda g: (0, 0, 0)),
            pl.BlockSpec((1536, 384), lambda g: (0, 0)),
        ],
        out_specs=pl.BlockSpec((8, 54, 128), lambda g: (g, 0, 0)),
        scratch_shapes=[pltpu.VMEM((9, 192, 128), F32)],
        cost_estimate=pl.CostEstimate(flops=3 * 10**9, bytes_accessed=9 * 10**6, transcendentals=0),
    )(fine, wt, mean)


def reg(ref, base, i, j):
    return ref[pl.ds((base + i * NJ + j) * 8, 8), :]


def put(ref, base, i, j, value):
    ref[pl.ds((base + i * NJ + j) * 8, 8), :] = value


def taken(ref, width, first, i, j):
    start = (i // 6) * width + first + 6 * j + i % 6
    return ref[pl.ds(start, 8, stride=4 * width), :]


def edges():
    sub = lax.broadcasted_iota(jnp.int32, (8, 128), 0)
    first, last = sub == 0, sub == 7
    north = lambda x: jnp.where(first, 0.0, pltpu.roll(x, 1, 0))
    south = lambda x: jnp.where(last, 0.0, pltpu.roll(x, 7, 0))
    return north, south


def west(row, j):
    return row[j - 1] if j else pltpu.roll(row[NJ - 1], 1, 1)


def east(row, j):
    return row[j + 1] if j + 1 < NJ else pltpu.roll(row[0], 127, 1)


def tangent_step(src, sb, dst, db, coef):
    north, south = edges()
    load = lambda i: [reg(src, sb, i, j) for j in range(NJ)]
    first, last = load(0), load(NI - 1)
    above = [north(x) for x in last]
    here = first
    for i in range(NI):
        below = load(i + 1) if i + 1 < NI else [south(x) for x in first]
        for j in range(NJ):
            put(
                dst,
                db,
                i,
                j,
                reg(coef, 0, i, j) * here[j]
                + reg(coef, REGS, i, j) * (above[j] + below[j] + east(here, j))
                + reg(coef, 2 * REGS, i, j) * west(here, j),
            )
        above, here = here, below


def adjoint_step(lam, coef, term):
    north, south = edges()

    def load(i):
        y = [reg(lam, 0, i, j) for j in range(NJ)]
        return y, [reg(coef, REGS, i, j) * y[j] for j in range(NJ)]

    above = [north(z) for z in load(NI - 1)[1]]
    y, here = load(0)
    wrap = [south(z) for z in here]
    for i in range(NI):
        y_next, below = load(i + 1) if i + 1 < NI else (None, wrap)
        both = [reg(coef, 2 * REGS, i, j) * y[j] for j in range(NJ)]
        new = [
            reg(coef, 0, i, j) * y[j] + (above[j] + below[j]) + (west(here, j) + east(both, j))
            for j in range(NJ)
        ]
        for j in range(NJ):
            add = term(i, j)
            put(lam, 0, i, j, new[j] if add is None else new[j] + add)
        above, here, y = here, below, y_next


def rhs_kernel(place_ref, own_ref, other_ref, f_ref, part_ref, coef_ref):
    core = place_ref[0]
    block = place_ref[1]

    def coefficients(diff_ref, cour_ref):
        for i in range(NI):
            for j in range(NJ):
                d = taken(diff_ref, 72, 0, i, j)
                c = taken(cour_ref, 72, 0, i, j)
                put(coef_ref, 0, i, j, 1.0 - 4.0 * d - c)
                put(coef_ref, REGS, i, j, d)
                put(coef_ref, 2 * REGS, i, j, d + c)

    @pl.when(core == 0)
    def _():
        coefficients(own_ref, other_ref)

    @pl.when(core != 0)
    def _():
        coefficients(other_ref, own_ref)

    for i in range(NI):
        for j in range(NJ):
            put(part_ref, 0, i, j, taken(f_ref, 54, 36, i, j))
    for t in (1, 0):
        adjoint_step(part_ref, coef_ref, lambda i, j: taken(f_ref, 54, 18 * t, i, j))

    def more(_, carry):
        adjoint_step(part_ref, coef_ref, lambda i, j: None)
        return carry

    lax.fori_loop(0, 3 * block, more, 0)


def rhs_part(place, own, other, f):
    return pl.pallas_call(
        rhs_kernel,
        name="rhs_part",
        out_shape=(
            jax.ShapeDtypeStruct((ROWS, 128), F32),
            jax.ShapeDtypeStruct((3 * ROWS, 128), F32),
        ),
        in_specs=[SMEM, VMEM, VMEM, VMEM],
        out_specs=(VMEM, VMEM),
        cost_estimate=pl.CostEstimate(flops=10**9, bytes_accessed=4 * 10**6, transcendentals=0),
    )(place, own.reshape(-1, 128), other.reshape(-1, 128), f.reshape(-1, 128))


def total(x):
    return jnp.sum(jnp.sum(x, axis=0, keepdims=True), axis=1, keepdims=True)


def ratio(a, b):
    return jnp.where(b > 0.0, a / jnp.where(b > 0.0, b, 1.0), 0.0)


def krylov_kernel(
    place_ref, p_ref, pc_ref, near_ref, far_ref, coef_ref, w0, w1, w2, w3, out_ref, v, xs, lam, wbuf
):
    core = place_ref[0]
    block = place_ref[1]
    for ref, flip in ((w0, 0), (w1, 1), (w2, 2), (w3, 3)):
        base = jnp.bitwise_xor(block, flip) * 3 * REGS
        for t in range(3):
            for i in range(NI):
                for j in range(NJ):
                    wbuf[pl.ds(pl.multiple_of((base + t * REGS + i * NJ + j) * 8, 8), 8), :] = taken(
                        ref, 72, 18 + 18 * t, i, j
                    )

    half = REGS // 2
    acc = jnp.zeros((8, 128), F32)

    def first(lo_ref, hi_ref):
        for r in range(REGS):
            far = lo_ref if r < half else hi_ref
            rows = pl.ds(r * 8, 8)
            v[rows, :] = (p_ref[rows, :] + pc_ref[rows, :]) + far[pl.ds((r % half) * 8, 8), :]

    @pl.when(core == 0)
    def _():
        first(near_ref, far_ref)

    @pl.when(core != 0)
    def _():
        first(far_ref, near_ref)

    for r in range(REGS):
        x = v[pl.ds(r * 8, 8), :]
        acc = acc + x * x

    lane = lax.broadcasted_iota(jnp.int32, (8, 128), 1)

    def product(k, carry):
        norm, before, table = carry
        base = pl.multiple_of(k * ROWS, 8)
        prev = pl.multiple_of(jnp.maximum(k - 1, 0) * ROWS, 8)
        for r in range(REGS):
            xs[pl.ds(r * 8, 8), :] = v[pl.ds(base + r * 8, 8), :]
        for t in range(STEPS - 1):
            tangent_step(xs, t * REGS, xs, (t + 1) * REGS, coef_ref)
        last = (STEPS - 1) * REGS
        for r in range(REGS):
            lam[pl.ds(r * 8, 8), :] = (
                wbuf[pl.ds((last + r) * 8, 8), :] * xs[pl.ds((last + r) * 8, 8), :]
            )
        for t in range(STEPS - 2, -1, -1):
            adjoint_step(
                lam,
                coef_ref,
                lambda i, j, t=t: reg(wbuf, t * REGS, i, j) * reg(xs, t * REGS, i, j),
            )
        dot = jnp.zeros((8, 128), F32)
        for r in range(REGS):
            x = xs[pl.ds(r * 8, 8), :]
            image = x + lam[pl.ds(r * 8, 8), :]
            lam[pl.ds(r * 8, 8), :] = image
            dot = dot + x * image
        a = ratio(total(dot), norm)
        b = jnp.where(k > 0, ratio(norm, before), 0.0)
        new = jnp.zeros((8, 128), F32)
        for r in range(REGS):
            x = (
                lam[pl.ds(r * 8, 8), :]
                - a * xs[pl.ds(r * 8, 8), :]
                - b * v[pl.ds(prev + r * 8, 8), :]
            )
            v[pl.ds(base + ROWS + r * 8, 8), :] = x
            new = new + x * x
        table = jnp.where(lane == k, norm, table)
        table = jnp.where(lane == k + 4, a, table)
        return total(new), norm, table

    one = jnp.ones((1, 1), F32)
    _, _, table = lax.fori_loop(
        0, ITERS, product, (total(acc), one, jnp.zeros((8, 128), F32))
    )
    for f in range(2):
        src = pl.multiple_of((core * 2 + f) * ROWS, 8)
        for i in range(NI):
            for j in range(NJ):
                start = (i // 6) * 40 + 18 * f + 6 * j + i % 6
                out_ref[pl.ds(start, 8, stride=160), :] = v[pl.ds(src + (i * NJ + j) * 8, 8), :]
    for s in range(32):
        out_ref[pl.ds(40 * s + 36, 4), :] = table[0:4]


def krylov(place, p, pc, near, far, coef, weights):
    return pl.pallas_call(
        krylov_kernel,
        name="krylov",
        out_shape=jax.ShapeDtypeStruct((32 * 40, 128), F32),
        in_specs=[SMEM] + [VMEM] * 9,
        out_specs=VMEM,
        scratch_shapes=[
            pltpu.VMEM((4 * ROWS, 128), F32),
            pltpu.VMEM((STEPS * ROWS, 128), F32),
            pltpu.VMEM((ROWS, 128), F32),
            pltpu.VMEM((STEPS * ROWS, 128), F32),
        ],
        cost_estimate=pl.CostEstimate(flops=10**9, bytes_accessed=8 * 10**6, transcendentals=0),
    )(place, p, pc, near, far, coef, *(w.reshape(-1, 128) for w in weights))


def small_cg(norms, diag):
    n = len(norms)
    zero = jnp.zeros_like(norms[0])
    off = [ratio(norms[k], norms[k - 1]) for k in range(1, n)]

    def image(p):
        q = []
        for k in range(n + 1):
            s = zero
            if k >= 1:
                s = s + p[k - 1]
            if k < n:
                s = s + diag[k] * p[k]
            if k + 1 < n:
                s = s + off[k] * p[k + 1]
            q.append(s)
        return q

    def dot(p, q):
        s = zero
        for k in range(n):
            s = s + norms[k] * p[k] * q[k]
        return jnp.sum(s, axis=0, keepdims=True)

    residual = [zero + 1.0] + [zero] * n
    direction = list(residual)
    control = [zero] * n
    rr = dot(residual, residual)
    for it in range(ITERS):
        h = image(direction)
        step = rr / dot(direction, h)
        control = [c + step * d for c, d in zip(control, direction)]
        residual = [r - step * x for r, x in zip(residual, h)]
        if it + 1 < ITERS:
            new = dot(residual, residual)
            direction = [r + new / rr * d for r, d in zip(residual, direction)]
            rr = new
    return control, residual


def finish_kernel(place_ref, own_ref, other_ref, spread_ref, back_ref, inc_ref, res_ref, tab, zc, zr):
    core = place_ref[0]
    block = place_ref[1]
    table = own_ref[pl.ds(36, 32, stride=40), :]
    control, residual = small_cg(
        [table[:, k : k + 1] for k in range(ITERS)],
        [table[:, 4 + k : 5 + k] for k in range(ITERS)],
    )
    lane = lax.broadcasted_iota(jnp.int32, (32, 128), 1)
    packed = jnp.zeros((32, 128), F32)
    for k, x in enumerate(control + residual):
        packed = jnp.where(lane == k, x, packed)
    tab[...] = packed
    mine = tab[pl.ds(pl.multiple_of(block * 8, 8), 8), :]

    def combine(pair):
        for m in range(8):
            coef = [mine[m : m + 1, k : k + 1] for k in range(7)]
            vs = []
            for k in range(4):
                if k // 2 == pair:
                    start = (block * 8 + m) * 40 + 18 * (k % 2)
                    vs.append([own_ref[pl.ds(start + 6 * j, 6), :] for j in range(NJ)])
                else:
                    start = m * 40 + 18 * (k % 2)
                    vs.append([other_ref[pl.ds(start + 6 * j, 6), :] for j in range(NJ)])
            for j in range(NJ):
                cols = pl.ds(128 * j, 128)
                zc[pl.ds(6 * m, 6), cols] = (
                    coef[0] * vs[0][j] + coef[1] * vs[1][j] + coef[2] * vs[2][j]
                )
                zr[pl.ds(6 * m, 6), cols] = (
                    coef[3] * vs[0][j]
                    + coef[4] * vs[1][j]
                    + coef[5] * vs[2][j]
                    + coef[6] * vs[3][j]
                )

    @pl.when(core == 0)
    def _():
        combine(0)

    @pl.when(core != 0)
    def _():
        combine(1)

    res = exact_dot(zr[...], back_ref[...])
    for m in range(8):
        res_ref[m] = res[6 * m : 6 * m + 6]
    inc = exact_dot(zc[...], spread_ref[...])
    for c in range(12):
        for e in range(4):
            inc_ref[c, pl.ds(e, 48, stride=4), :] = inc[:, 128 * c : 128 * c + 128]


def finish_body(place_ref, own_ref, other_ref, spread_ref, back_ref, inc_ref, res_ref, tab, zc, zr, wide):
    finish_kernel(place_ref, own_ref, other_ref, spread_ref, back_ref, wide, res_ref, tab, zc, zr)
    for c in range(12):
        inc_ref[:, 128 * c : 128 * c + 128] = wide[c]


def finish(place, own, other, spread, back):
    return pl.pallas_call(
        finish_body,
        name="finish",
        out_shape=(
            jax.ShapeDtypeStruct((192, 1536), F32),
            jax.ShapeDtypeStruct((8, 6, 384), F32),
        ),
        in_specs=[SMEM, VMEM, VMEM, VMEM, VMEM],
        out_specs=(VMEM, VMEM),
        scratch_shapes=[
            pltpu.VMEM((32, 128), F32),
            pltpu.VMEM((48, 384), F32),
            pltpu.VMEM((48, 384), F32),
            pltpu.VMEM((12, 192, 128), F32),
        ],
        cost_estimate=pl.CostEstimate(flops=10**9, bytes_accessed=4 * 10**6, transcendentals=0),
    )(place, own, other.reshape(-1, 128), spread, back)


def on_device(innovations, obs_counts, diffusion, courant):
    core = lax.axis_index("tm_1")
    block = lax.axis_index(TM)
    place = jnp.stack([core, block]).astype(jnp.int32)
    pick, mean, spread, back = matrices()
    swap = lambda x, axis: lax.ppermute(x, axis, SWAP)
    turn = lambda x: lax.all_to_all(x, SPACE, 0, 0, tiled=True)

    chunks, wt = prepare(place, obs_counts, diffusion, courant, pick)
    own = turn(chunks)
    forcing = restrict(innovations.reshape(3, 768, 1536), wt, mean)
    pair = swap(own, "tm_1")
    across = swap(own, "tm_0")
    across_pair = swap(across, "tm_1")
    f = turn(forcing)
    p, coef = rhs_part(place, own, pair, f)
    pc = swap(p, "tm_1")
    half = ROWS // 2
    mine = lax.dynamic_slice_in_dim(p, core * half, half, 0) + lax.dynamic_slice_in_dim(
        pc, core * half, half, 0
    )
    near = swap(mine, "tm_0")
    far = swap(near, "tm_1")
    out = turn(
        krylov(place, p, pc, near, far, coef, (own, pair, across, across_pair)).reshape(32, 40, 128)
    )
    other = swap(
        lax.dynamic_slice_in_dim(out, (block + 1 - 2 * core) * 8, 8, 0), "tm_1"
    )
    increment, residual = finish(place, out.reshape(-1, 128), other, spread, back)
    return (increment.reshape(8, 24, 1536), residual)


def solution(mesh):
    torus = Mesh(
        mesh.devices.reshape(2, 4, 4, 2, 2), ("space_0", "space_1", "space_2", "tm_0", "tm_1")
    )
    return jax.shard_map(
        on_device,
        mesh=torus,
        in_specs=(
            P(TM, None, SPACE, None),
            P(TM, SPACE, None),
            P(None, SPACE, None),
            P(None, SPACE, None),
        ),
        out_specs=(P(TM, SPACE, None), P(TM, SPACE, None)),
        check_vma=False,
    )
```

```python
import jax
import jax.numpy as jnp
from jax import lax
from jax.experimental import pallas as pl
from jax.experimental.pallas import tpu as pltpu
from jax.sharding import Mesh
from jax.sharding import PartitionSpec as P

SPACE = ("space_0", "space_1", "space_2")
TURN = ("space_2", "space_0", "space_1")
TM = ("tm_0", "tm_1")
SWAP = [(0, 1), (1, 0)]
F32 = jnp.float32
BF16 = jnp.bfloat16

NI, NJ = 24, 3
REGS = NI * NJ
ROWS = REGS * 8
STEPS = 12
ITERS = 3
AT_F, AT_W, WIDTH = 18, 72, 184
FIELD = 24
BACK = 40
VMEM = pl.BlockSpec(memory_space=pltpu.VMEM)
SMEM = pl.BlockSpec(memory_space=pltpu.SMEM)
ANY = pl.BlockSpec(memory_space=pl.ANY)


def params(mib):
    return pltpu.CompilerParams(vmem_limit_bytes=mib * 2**20)


def cost(us):
    return pl.CostEstimate(flops=int(us * 10**7), bytes_accessed=10**6, transcendentals=0)


def lanes(shape):
    return lax.broadcasted_iota(jnp.int32, shape, 1)


def pick(index, blocks, which, shape):
    out = None
    for k, x in enumerate(blocks):
        y = jnp.take_along_axis(x, index, axis=1, mode="promise_in_bounds")
        out = y if out is None else jnp.where(which == k, y, out)
    return out


def to_held(blocks):
    shape = blocks[0].shape
    out = []
    for j in range(NJ):
        column = lanes(shape) * NJ + j
        out.append(pick(column & 127, blocks, column >> 7, shape))
    return out


def to_natural(held, b, repeat):
    shape = held[0].shape
    column = (lanes(shape) + 128 * b) // repeat
    lane = (column * 43691) >> 17
    return pick(lane, held, column - lane * NJ, shape)


def scatter_kernel(
    place_ref, counts_ref, across_ref, diff_ref, cour_ref, fine_ref, out_ref, mean_ref, sums_ref, w_ref
):
    @pl.when(pl.program_id(0) == 0)
    def _():
        shape = (512, 128)
        row = lax.broadcasted_iota(jnp.int32, shape, 0)
        mean_ref[...] = jnp.where((row >> 2) == lanes(shape), 1.0 / 16.0, 0.0).astype(BF16)
        for half, ref in enumerate((counts_ref, across_ref)):
            for t in range(3):
                w = to_held([ref[t, :, 128 * b : 128 * b + 128].astype(F32) for b in range(3)])
                for j in range(NJ):
                    w_ref[pl.ds((half * 3 + t) * 24 + 8 * j, 6), :] = w[j]

    def store(row, value):
        out_ref[pl.ds(row, 8, stride=WIDTH), :] = value

    core = place_ref[0]
    for i in range(6):
        blocks = [
            jnp.where(
                core == 0,
                diff_ref[i, :, 128 * b : 128 * b + 128],
                cour_ref[i, :, 128 * b : 128 * b + 128],
            )
            for b in range(3)
        ]
        for j, x in enumerate(to_held(blocks)):
            store(6 * j + i, x)
    for t in range(3):
        for b in range(3):
            sums_ref[3 * t + b] = jnp.dot(
                fine_ref[t, :, 512 * b : 512 * b + 512],
                mean_ref[...],
                preferred_element_type=F32,
            )
        for i in range(6):
            blocks = [
                (
                    sums_ref[3 * t + b, pl.ds(4 * i, 8, stride=24), :]
                    + sums_ref[3 * t + b, pl.ds(4 * i + 1, 8, stride=24), :]
                )
                + (
                    sums_ref[3 * t + b, pl.ds(4 * i + 2, 8, stride=24), :]
                    + sums_ref[3 * t + b, pl.ds(4 * i + 3, 8, stride=24), :]
                )
                for b in range(3)
            ]
            for j, x in enumerate(to_held(blocks)):
                row = 6 * j + i
                for half in range(2):
                    w = jnp.broadcast_to(w_ref[pl.ds((half * 3 + t) * 24 + 8 * j + i, 1), :], (8, 128))
                    store(AT_W + (half * 3 + t) * 18 + row, w)
                    if half == 0:
                        store(AT_F + 18 * t + row, w * x)


def scatter(place, counts, across, diffusion, courant, fine):
    return pl.pallas_call(
        scatter_kernel,
        name="scatter",
        grid=(4,),
        out_shape=jax.ShapeDtypeStruct((32 * WIDTH, 128), F32),
        in_specs=[
            SMEM,
            pl.BlockSpec((3, 6, 384), lambda g: (0, 0, 0)),
            pl.BlockSpec((3, 6, 384), lambda g: (0, 0, 0)),
            pl.BlockSpec((6, 8, 384), lambda g: (0, g, 0)),
            pl.BlockSpec((6, 8, 384), lambda g: (0, g, 0)),
            pl.BlockSpec((3, 192, 1536), lambda g: (0, g, 0)),
        ],
        out_specs=pl.BlockSpec((8 * WIDTH, 128), lambda g: (g, 0)),
        scratch_shapes=[
            pltpu.VMEM((512, 128), BF16),
            pltpu.VMEM((9, 192, 128), F32),
            pltpu.VMEM((144, 128), F32),
        ],
        compiler_params=params(24),
        cost_estimate=cost(8),
    )(place, counts, across, diffusion, courant, fine)


def reg(ref, base, i, j):
    return ref[pl.ds((base + i * NJ + j) * 8, 8), :]


def put(ref, base, i, j, value):
    ref[pl.ds((base + i * NJ + j) * 8, 8), :] = value


def taken(ref, width, first, i, j):
    return ref[pl.ds((i // 6) * 8 * width + first + 6 * j + i % 6, 8, stride=width), :]


def edges():
    sub = lax.broadcasted_iota(jnp.int32, (8, 128), 0)
    first, last = sub == 0, sub == 7
    north = lambda x: jnp.where(first, 0.0, pltpu.roll(x, 1, 0))
    south = lambda x: jnp.where(last, 0.0, pltpu.roll(x, 7, 0))
    return north, south


def west(row, j):
    return row[j - 1] if j else pltpu.roll(row[NJ - 1], 1, 1)


def east(row, j):
    return row[j + 1] if j + 1 < NJ else pltpu.roll(row[0], 127, 1)


def tangent_step(src, sb, dst, db, coef):
    north, south = edges()
    load = lambda i: [reg(src, sb, i, j) for j in range(NJ)]
    first, last = load(0), load(NI - 1)
    above = [north(x) for x in last]
    here = first
    for i in range(NI):
        below = load(i + 1) if i + 1 < NI else [south(x) for x in first]
        for j in range(NJ):
            put(
                dst,
                db,
                i,
                j,
                reg(coef, 0, i, j) * here[j]
                + reg(coef, REGS, i, j) * (above[j] + below[j] + east(here, j))
                + reg(coef, 2 * REGS, i, j) * west(here, j),
            )
        above, here = here, below


def adjoint_step(lam, coef, term):
    north, south = edges()

    def load(i):
        y = [reg(lam, 0, i, j) for j in range(NJ)]
        return y, [reg(coef, REGS, i, j) * y[j] for j in range(NJ)]

    above = [north(z) for z in load(NI - 1)[1]]
    y, here = load(0)
    wrap = [south(z) for z in here]
    for i in range(NI):
        y_next, below = load(i + 1) if i + 1 < NI else (None, wrap)
        both = [reg(coef, 2 * REGS, i, j) * y[j] for j in range(NJ)]
        new = [
            reg(coef, 0, i, j) * y[j] + (above[j] + below[j]) + (west(here, j) + east(both, j))
            for j in range(NJ)
        ]
        for j in range(NJ):
            add = term(i, j)
            put(lam, 0, i, j, new[j] if add is None else new[j] + add)
        above, here, y = here, below, y_next


def rhs_kernel(place_ref, own_ref, other_ref, keep_ref, send_ref, coef_ref, lam):
    core = place_ref[0]
    block = place_ref[1]

    def coefficients(diff_ref, diff_width, cour_ref, cour_width):
        for i in range(NI):
            for j in range(NJ):
                d = taken(diff_ref, diff_width, 0, i, j)
                c = taken(cour_ref, cour_width, 0, i, j)
                put(coef_ref, 0, i, j, 1.0 - 4.0 * d - c)
                put(coef_ref, REGS, i, j, d)
                put(coef_ref, 2 * REGS, i, j, d + c)

    @pl.when(core == 0)
    def _():
        coefficients(own_ref, WIDTH, other_ref, FIELD)

    @pl.when(core != 0)
    def _():
        coefficients(other_ref, FIELD, own_ref, WIDTH)

    for i in range(NI):
        for j in range(NJ):
            put(lam, 0, i, j, taken(own_ref, WIDTH, AT_F + 36, i, j))
    for t in (1, 0):
        adjoint_step(lam, coef_ref, lambda i, j, t=t: taken(own_ref, WIDTH, AT_F + 18 * t, i, j))

    def more(_, carry):
        adjoint_step(lam, coef_ref, lambda i, j: None)
        return carry

    lax.fori_loop(0, 3 * block, more, 0)
    half = ROWS // 2
    keep_ref[...] = lam[pl.ds(pl.multiple_of(core * half, 8), half), :]
    send_ref[...] = lam[pl.ds(pl.multiple_of((1 - core) * half, 8), half), :]


def rhs_part(place, own, other):
    return pl.pallas_call(
        rhs_kernel,
        name="rhs_part",
        out_shape=(
            jax.ShapeDtypeStruct((ROWS // 2, 128), F32),
            jax.ShapeDtypeStruct((ROWS // 2, 128), F32),
            jax.ShapeDtypeStruct((3 * ROWS, 128), F32),
        ),
        in_specs=[SMEM, VMEM, VMEM],
        out_specs=(VMEM, VMEM, VMEM),
        scratch_shapes=[pltpu.VMEM((ROWS, 128), F32)],
        compiler_params=params(16),
        cost_estimate=cost(4),
    )(place, own, other.reshape(-1, 128))


def weights_kernel(place_ref, own_ref, pair_ref, out_ref):
    block = place_ref[1]
    for ref, flip in ((own_ref, 0), (pair_ref, 1)):
        for half in range(2):
            base = jnp.bitwise_xor(block, flip + 2 * half) * 3 * REGS
            for t in range(3):
                for i in range(NI):
                    for j in range(NJ):
                        row = pl.multiple_of((base + t * REGS + i * NJ + j) * 8, 8)
                        out_ref[pl.ds(row, 8), :] = taken(
                            ref, WIDTH, AT_W + (3 * half + t) * 18, i, j
                        )


def weights(place, own, pair):
    return pl.pallas_call(
        weights_kernel,
        name="weights",
        out_shape=jax.ShapeDtypeStruct((STEPS * ROWS, 128), F32),
        in_specs=[SMEM, VMEM, VMEM],
        out_specs=VMEM,
        compiler_params=params(24),
        cost_estimate=cost(4),
    )(place, own, pair)


def total(x):
    return jnp.sum(jnp.sum(x, axis=0, keepdims=True), axis=1, keepdims=True)


def ratio(a, b):
    return jnp.where(b > 0.0, a / jnp.where(b > 0.0, b, 1.0), 0.0)


def krylov_kernel(place_ref, mine_ref, other_ref, coef_ref, w_ref, out_ref, v, xs, lam, wbuf, sem):
    core = place_ref[0]
    fetch = pltpu.make_async_copy(w_ref, wbuf, sem)
    fetch.start()
    half = REGS // 2

    def first(lo_ref, hi_ref):
        acc = jnp.zeros((8, 128), F32)
        for r in range(REGS):
            x = (lo_ref if r < half else hi_ref)[pl.ds((r % half) * 8, 8), :]
            v[pl.ds(r * 8, 8), :] = x
            acc = acc + x * x
        lam[pl.ds(0, 8), :] = acc

    @pl.when(core == 0)
    def _():
        first(mine_ref, other_ref)

    @pl.when(core != 0)
    def _():
        first(other_ref, mine_ref)

    norm0 = total(lam[pl.ds(0, 8), :])
    lane = lanes((8, 128))

    def product(k, carry):
        norm, before, table = carry
        base = pl.multiple_of(k * ROWS, 8)
        prev = pl.multiple_of(jnp.maximum(k - 1, 0) * ROWS, 8)
        for r in range(REGS):
            xs[pl.ds(r * 8, 8), :] = v[pl.ds(base + r * 8, 8), :]
        for t in range(STEPS - 1):
            tangent_step(xs, t * REGS, xs, (t + 1) * REGS, coef_ref)

        @pl.when(k == 0)
        def _():
            fetch.wait()

        last = (STEPS - 1) * REGS
        for r in range(REGS):
            lam[pl.ds(r * 8, 8), :] = (
                wbuf[pl.ds((last + r) * 8, 8), :] * xs[pl.ds((last + r) * 8, 8), :]
            )
        for t in range(STEPS - 2, -1, -1):
            adjoint_step(
                lam,
                coef_ref,
                lambda i, j, t=t: reg(wbuf, t * REGS, i, j) * reg(xs, t * REGS, i, j),
            )
        dot = jnp.zeros((8, 128), F32)
        for r in range(REGS):
            x = xs[pl.ds(r * 8, 8), :]
            image = x + lam[pl.ds(r * 8, 8), :]
            lam[pl.ds(r * 8, 8), :] = image
            dot = dot + x * image
        a = ratio(total(dot), norm)
        b = jnp.where(k > 0, ratio(norm, before), 0.0)
        new = jnp.zeros((8, 128), F32)
        for r in range(REGS):
            x = (
                lam[pl.ds(r * 8, 8), :]
                - a * xs[pl.ds(r * 8, 8), :]
                - b * v[pl.ds(prev + r * 8, 8), :]
            )
            v[pl.ds(base + ROWS + r * 8, 8), :] = x
            new = new + x * x
        table = jnp.where(lane == k, norm, table)
        table = jnp.where(lane == k + 4, a, table)
        return total(new), norm, table

    _, _, table = lax.fori_loop(
        0, ITERS, product, (norm0, jnp.ones((1, 1), F32), jnp.zeros((8, 128), F32))
    )
    for f in range(2):
        src = pl.multiple_of((core * 2 + f) * ROWS, 8)
        for i in range(NI):
            for j in range(NJ):
                start = (i // 6) * 8 * BACK + 18 * f + 6 * j + i % 6
                out_ref[pl.ds(start, 8, stride=BACK), :] = v[pl.ds(src + (i * NJ + j) * 8, 8), :]
    for g in range(4):
        out_ref[pl.ds(8 * BACK * g + 36, 8, stride=BACK), :] = table


def krylov(place, mine, other, coef, w):
    return pl.pallas_call(
        krylov_kernel,
        name="krylov",
        out_shape=jax.ShapeDtypeStruct((32 * BACK, 128), F32),
        in_specs=[SMEM, VMEM, VMEM, VMEM, ANY],
        out_specs=VMEM,
        scratch_shapes=[
            pltpu.VMEM((4 * ROWS, 128), F32),
            pltpu.VMEM((STEPS * ROWS, 128), F32),
            pltpu.VMEM((ROWS, 128), F32),
            pltpu.VMEM((STEPS * ROWS, 128), F32),
            pltpu.SemaphoreType.DMA,
        ],
        compiler_params=params(24),
        cost_estimate=cost(12),
    )(place, mine, other, coef, w)


def small_cg(norms, diag):
    n = len(norms)
    zero = jnp.zeros_like(norms[0])
    off = [ratio(norms[k], norms[k - 1]) for k in range(1, n)]

    def image(p):
        q = []
        for k in range(n + 1):
            s = zero
            if k >= 1:
                s = s + p[k - 1]
            if k < n:
                s = s + diag[k] * p[k]
            if k + 1 < n:
                s = s + off[k] * p[k + 1]
            q.append(s)
        return q

    def dot(p, q):
        s = zero
        for k in range(n):
            s = s + norms[k] * p[k] * q[k]
        return jnp.sum(s, axis=0, keepdims=True)

    residual = [zero + 1.0] + [zero] * n
    direction = list(residual)
    control = [zero] * n
    rr = dot(residual, residual)
    for it in range(ITERS):
        h = image(direction)
        step = rr / dot(direction, h)
        control = [c + step * d for c, d in zip(control, direction)]
        residual = [r - step * x for r, x in zip(residual, h)]
        if it + 1 < ITERS:
            new = dot(residual, residual)
            direction = [r + new / rr * d for r, d in zip(residual, direction)]
            rr = new
    return control, residual


def finish_kernel(place_ref, own_ref, other_ref, inc_ref, res_ref, tab, wide):
    core = place_ref[0]
    block = place_ref[1]
    table = own_ref[pl.ds(36, 32, stride=BACK), :]
    control, residual = small_cg(
        [table[:, k : k + 1] for k in range(ITERS)],
        [table[:, 4 + k : 5 + k] for k in range(ITERS)],
    )
    lane = lanes((32, 128))
    packed = jnp.zeros((32, 128), F32)
    for k, x in enumerate(control + residual):
        packed = jnp.where(lane == k, x, packed)
    tab[...] = packed
    mine = tab[pl.ds(pl.multiple_of(block * 8, 8), 8), :]
    coef = [jnp.broadcast_to(mine[:, k : k + 1], (8, 128)) for k in range(7)]
    here = block * 8 * BACK

    def fields(i, j):
        out = []
        for k in range(4):
            row = 18 * (k % 2) + 6 * j + i
            a = own_ref[pl.ds(here + row, 8, stride=BACK), :]
            b = other_ref[pl.ds(row, 8, stride=BACK), :]
            out.append(jnp.where(core == k // 2, a, b))
        return out

    for i in range(6):
        inc, res = [], []
        for j in range(NJ):
            v = fields(i, j)
            inc.append(coef[0] * v[0] + coef[1] * v[1] + coef[2] * v[2])
            res.append(coef[3] * v[0] + coef[4] * v[1] + coef[5] * v[2] + coef[6] * v[3])
        for b in range(3):
            res_ref[i, :, 128 * b : 128 * b + 128] = to_natural(res, b, 1)
        for b in range(12):
            x = to_natural(inc, b, 4)
            for e in range(4):
                wide[b, pl.ds(4 * i + e, 8, stride=24), :] = x
    for b in range(12):
        inc_ref[:, 128 * b : 128 * b + 128] = wide[b]


def finish(place, own, other):
    return pl.pallas_call(
        finish_kernel,
        name="finish",
        out_shape=(
            jax.ShapeDtypeStruct((192, 1536), F32),
            jax.ShapeDtypeStruct((6, 8, 384), F32),
        ),
        in_specs=[SMEM, VMEM, VMEM],
        out_specs=(VMEM, VMEM),
        scratch_shapes=[pltpu.VMEM((32, 128), F32), pltpu.VMEM((12, 192, 128), F32)],
        compiler_params=params(16),
        cost_estimate=cost(3),
    )(place, own, other.reshape(-1, 128))


def on_device(innovations, obs_counts, diffusion, courant):
    core = lax.axis_index("tm_1")
    block = lax.axis_index(TM)
    place = jnp.stack([core, block]).astype(jnp.int32)
    swap = lambda x, axis: lax.ppermute(x, axis, SWAP)
    turn = lambda x: lax.all_to_all(x.reshape(32, -1, 128), TURN, 0, 0, tiled=True)

    own = turn(
        scatter(
            place,
            obs_counts,
            swap(obs_counts, "tm_0"),
            jnp.transpose(diffusion, (1, 0, 2)),
            jnp.transpose(courant, (1, 0, 2)),
            innovations.reshape(3, 768, 1536),
        )
    )
    other = swap(own[:, :FIELD], "tm_1")
    flat = own.reshape(-1, 128)
    pair = swap(flat, "tm_1")
    keep, send, coef = rhs_part(place, flat, other)
    w = weights(place, flat, pair)
    part = keep + swap(send, "tm_1")
    mine = part + swap(part, "tm_0")
    out = turn(krylov(place, mine, swap(mine, "tm_1"), coef, w))
    theirs = swap(lax.dynamic_slice_in_dim(out, (block + 1 - 2 * core) * 8, 8, 0), "tm_1")
    increment, residual = finish(place, out.reshape(-1, 128), theirs)
    return (increment.reshape(8, 24, 1536), jnp.transpose(residual, (1, 0, 2)))


def solution(mesh):
    torus = Mesh(
        mesh.devices.reshape(2, 4, 4, 2, 2), ("space_0", "space_1", "space_2", "tm_0", "tm_1")
    )
    return jax.shard_map(
        on_device,
        mesh=torus,
        in_specs=(
            P(TM, None, SPACE, None),
            P(TM, SPACE, None),
            P(None, SPACE, None),
            P(None, SPACE, None),
        ),
        out_specs=(P(TM, SPACE, None), P(TM, SPACE, None)),
        check_vma=False,
    )
```

```python
import jax
import jax.numpy as jnp
from jax import lax
from jax.experimental import pallas as pl
from jax.experimental.pallas import tpu as pltpu
from jax.sharding import Mesh
from jax.sharding import PartitionSpec as P

SPACE = ("space_0", "space_1", "space_2")
TURN = ("space_2", "space_0", "space_1")
TM = ("tm_0", "tm_1")
SWAP = [(0, 1), (1, 0)]
F32 = jnp.float32
BF16 = jnp.bfloat16

NI, NJ = 24, 3
REGS = NI * NJ
ROWS = REGS * 8
STEPS = 12
ITERS = 3
AT_F, WIDTH = 18, 72
PIECE = 56
FIELD = 24
BACK = 40
VMEM = pl.BlockSpec(memory_space=pltpu.VMEM)
SMEM = pl.BlockSpec(memory_space=pltpu.SMEM)
ANY = pl.BlockSpec(memory_space=pl.ANY)


def params(mib):
    return pltpu.CompilerParams(vmem_limit_bytes=mib * 2**20)


def cost(us):
    return pl.CostEstimate(flops=int(us * 10**7), bytes_accessed=10**6, transcendentals=0)


def lanes(shape):
    return lax.broadcasted_iota(jnp.int32, shape, 1)


def pick(index, blocks, which):
    out = None
    for k, x in enumerate(blocks):
        y = jnp.take_along_axis(x, index, axis=1, mode="promise_in_bounds")
        out = y if out is None else jnp.where(which == k, y, out)
    return out


def to_held(blocks):
    shape = blocks[0].shape
    out = []
    for j in range(NJ):
        column = lanes(shape) * NJ + j
        out.append(pick(column & 127, blocks, column >> 7))
    return out


def to_natural(held, b, repeat):
    shape = held[0].shape
    column = (lanes(shape) + 128 * b) // repeat
    lane = (column * 43691) >> 17
    return pick(lane, held, column - lane * NJ)


def held_kernel(counts_ref, out_ref):
    for t in range(3):
        w = to_held([counts_ref[t, :, 128 * b : 128 * b + 128].astype(F32) for b in range(3)])
        for j in range(NJ):
            out_ref[pl.ds(18 * t + 6 * j, 6), :] = w[j]
    out_ref[pl.ds(54, 2), :] = jnp.zeros((2, 128), F32)


def held(counts):
    return pl.pallas_call(
        held_kernel,
        name="held",
        out_shape=jax.ShapeDtypeStruct((PIECE, 128), F32),
        in_specs=[VMEM],
        out_specs=VMEM,
        compiler_params=params(4),
        cost_estimate=cost(0.5),
    )(counts)


def scatter_kernel(
    place_ref, w_ref, diff_ref, cour_ref, fine_ref, out_ref, mean_ref, sums_ref
):
    @pl.when(pl.program_id(0) == 0)
    def _():
        shape = (512, 128)
        row = lax.broadcasted_iota(jnp.int32, shape, 0)
        mean_ref[...] = jnp.where((row >> 2) == lanes(shape), 1.0 / 16.0, 0.0).astype(BF16)

    def store(row, value):
        out_ref[pl.ds(row, 8, stride=WIDTH), :] = value

    core = place_ref[0]
    for i in range(6):
        blocks = [
            jnp.where(
                core == 0,
                diff_ref[i, :, 128 * b : 128 * b + 128],
                cour_ref[i, :, 128 * b : 128 * b + 128],
            )
            for b in range(3)
        ]
        for j, x in enumerate(to_held(blocks)):
            store(6 * j + i, x)
    for t in range(3):
        for b in range(3):
            sums_ref[3 * t + b] = jnp.dot(
                fine_ref[t, :, 512 * b : 512 * b + 512],
                mean_ref[...],
                preferred_element_type=F32,
            )
        for i in range(6):
            blocks = [
                (
                    sums_ref[3 * t + b, pl.ds(4 * i, 8, stride=24), :]
                    + sums_ref[3 * t + b, pl.ds(4 * i + 1, 8, stride=24), :]
                )
                + (
                    sums_ref[3 * t + b, pl.ds(4 * i + 2, 8, stride=24), :]
                    + sums_ref[3 * t + b, pl.ds(4 * i + 3, 8, stride=24), :]
                )
                for b in range(3)
            ]
            for j, x in enumerate(to_held(blocks)):
                row = 18 * t + 6 * j + i
                w = jnp.broadcast_to(w_ref[pl.ds(row, 1), :], (8, 128))
                store(AT_F + row, w * x)


def scatter(place, w, diffusion, courant, fine):
    return pl.pallas_call(
        scatter_kernel,
        name="scatter",
        grid=(4,),
        out_shape=jax.ShapeDtypeStruct((32 * WIDTH, 128), F32),
        in_specs=[
            SMEM,
            pl.BlockSpec((PIECE, 128), lambda g: (0, 0)),
            pl.BlockSpec((6, 8, 384), lambda g: (0, g, 0)),
            pl.BlockSpec((6, 8, 384), lambda g: (0, g, 0)),
            pl.BlockSpec((3, 192, 1536), lambda g: (0, g, 0)),
        ],
        out_specs=pl.BlockSpec((8 * WIDTH, 128), lambda g: (g, 0)),
        scratch_shapes=[
            pltpu.VMEM((512, 128), BF16),
            pltpu.VMEM((9, 192, 128), F32),
        ],
        compiler_params=params(57),
        cost_estimate=cost(8),
    )(place, w, diffusion, courant, fine)


def reg(ref, base, i, j):
    return ref[pl.ds((base + i * NJ + j) * 8, 8), :]


def put(ref, base, i, j, value):
    ref[pl.ds((base + i * NJ + j) * 8, 8), :] = value


def taken(ref, width, first, i, j):
    return ref[pl.ds((i // 6) * 8 * width + first + 6 * j + i % 6, 8, stride=width), :]


def edges():
    sub = lax.broadcasted_iota(jnp.int32, (8, 128), 0)
    first, last = sub == 0, sub == 7
    north = lambda x: jnp.where(first, 0.0, pltpu.roll(x, 1, 0))
    south = lambda x: jnp.where(last, 0.0, pltpu.roll(x, 7, 0))
    return north, south


def west(row, j):
    return row[j - 1] if j else pltpu.roll(row[NJ - 1], 1, 1)


def east(row, j):
    return row[j + 1] if j + 1 < NJ else pltpu.roll(row[0], 127, 1)


def tangent_step(src, sb, dst, db, coef):
    north, south = edges()
    load = lambda i: [reg(src, sb, i, j) for j in range(NJ)]
    first, last = load(0), load(NI - 1)
    above = [north(x) for x in last]
    here = first
    for i in range(NI):
        below = load(i + 1) if i + 1 < NI else [south(x) for x in first]
        for j in range(NJ):
            put(
                dst,
                db,
                i,
                j,
                reg(coef, 0, i, j) * here[j]
                + reg(coef, REGS, i, j) * (above[j] + below[j] + east(here, j))
                + reg(coef, 2 * REGS, i, j) * west(here, j),
            )
        above, here = here, below


def adjoint_step(lam, coef, term):
    north, south = edges()

    def load(i):
        y = [reg(lam, 0, i, j) for j in range(NJ)]
        return y, [reg(coef, REGS, i, j) * y[j] for j in range(NJ)]

    above = [north(z) for z in load(NI - 1)[1]]
    y, here = load(0)
    wrap = [south(z) for z in here]
    for i in range(NI):
        y_next, below = load(i + 1) if i + 1 < NI else (None, wrap)
        both = [reg(coef, 2 * REGS, i, j) * y[j] for j in range(NJ)]
        new = [
            reg(coef, 0, i, j) * y[j] + (above[j] + below[j]) + (west(here, j) + east(both, j))
            for j in range(NJ)
        ]
        for j in range(NJ):
            add = term(i, j)
            put(lam, 0, i, j, new[j] if add is None else new[j] + add)
        above, here, y = here, below, y_next


def rhs_kernel(place_ref, own_ref, other_ref, keep_ref, send_ref, coef_ref, lam):
    core = place_ref[0]
    block = place_ref[1]

    def coefficients(diff_ref, diff_width, cour_ref, cour_width):
        for i in range(NI):
            for j in range(NJ):
                d = taken(diff_ref, diff_width, 0, i, j)
                c = taken(cour_ref, cour_width, 0, i, j)
                put(coef_ref, 0, i, j, 1.0 - 4.0 * d - c)
                put(coef_ref, REGS, i, j, d)
                put(coef_ref, 2 * REGS, i, j, d + c)

    @pl.when(core == 0)
    def _():
        coefficients(own_ref, WIDTH, other_ref, FIELD)

    @pl.when(core != 0)
    def _():
        coefficients(other_ref, FIELD, own_ref, WIDTH)

    for i in range(NI):
        for j in range(NJ):
            put(lam, 0, i, j, taken(own_ref, WIDTH, AT_F + 36, i, j))
    for t in (1, 0):
        adjoint_step(lam, coef_ref, lambda i, j, t=t: taken(own_ref, WIDTH, AT_F + 18 * t, i, j))

    def more(_, carry):
        adjoint_step(lam, coef_ref, lambda i, j: None)
        return carry

    lax.fori_loop(0, 3 * block, more, 0)
    half = ROWS // 2
    keep_ref[...] = lam[pl.ds(pl.multiple_of(core * half, 8), half), :]
    send_ref[...] = lam[pl.ds(pl.multiple_of((1 - core) * half, 8), half), :]


def rhs_part(place, own, other):
    return pl.pallas_call(
        rhs_kernel,
        name="rhs_part",
        out_shape=(
            jax.ShapeDtypeStruct((ROWS // 2, 128), F32),
            jax.ShapeDtypeStruct((ROWS // 2, 128), F32),
            jax.ShapeDtypeStruct((3 * ROWS, 128), F32),
        ),
        in_specs=[SMEM, VMEM, VMEM],
        out_specs=(VMEM, VMEM, VMEM),
        scratch_shapes=[pltpu.VMEM((ROWS, 128), F32)],
        compiler_params=params(16),
        cost_estimate=cost(4),
    )(place, own, other.reshape(-1, 128))


def weights_kernel(place_ref, *refs):
    out_ref = refs[-1]
    block, row = place_ref[1], place_ref[2]
    for core in range(2):
        for d in range(4):
            ref = refs[4 * core + d]
            first = jnp.bitwise_and(row + d, 3) * 6 * NJ
            for half in range(2):
                base = jnp.bitwise_xor(block, core + 2 * half) * 3 * REGS + first
                for t in range(3):
                    for i in range(6):
                        for j in range(NJ):
                            at = pl.multiple_of((base + t * REGS + i * NJ + j) * 8, 8)
                            start = PIECE * half + 18 * t + 6 * j + i
                            out_ref[pl.ds(at, 8), :] = ref[pl.ds(start, 8, stride=2 * PIECE), :]


def weights(place, pieces):
    return pl.pallas_call(
        weights_kernel,
        name="weights",
        out_shape=jax.ShapeDtypeStruct((STEPS * ROWS, 128), F32),
        in_specs=[SMEM] + [VMEM] * 8,
        out_specs=VMEM,
        compiler_params=params(16),
        cost_estimate=cost(4),
    )(place, *pieces)


def shift(x, axis, by):
    return lax.ppermute(x, axis, [(k, (k + by) % 4) for k in range(4)])


def swap(x, axis):
    return lax.ppermute(x, axis, SWAP)


def crossed(w):
    both = lax.ppermute(w, ("space_0", "tm_0"), [(k, 3 - k) for k in range(4)])
    x = jnp.concatenate([w, swap(w, "tm_0")], 0)
    y = jnp.concatenate([swap(w, "space_0"), both], 0)
    low = lax.axis_index("space_0") == 0
    return jnp.stack([jnp.where(low, x, y), jnp.where(low, y, x)])


def lined(x):
    behind, ahead, far = (shift(x, "space_1", by) for by in (1, -1, 2))
    around = jnp.stack([x, ahead, far, behind, x, ahead, far, behind], 1)
    start = jnp.bitwise_and(4 - lax.axis_index("space_1"), 3)
    return lax.dynamic_slice_in_dim(around, start, 4, 1).reshape(2, -1, 128)


def total(x):
    return jnp.sum(jnp.sum(x, axis=0, keepdims=True), axis=1, keepdims=True)


def ratio(a, b):
    return jnp.where(b > 0.0, a / jnp.where(b > 0.0, b, 1.0), 0.0)


def krylov_kernel(place_ref, mine_ref, other_ref, coef_ref, w_ref, out_ref, v, xs, lam, wbuf, sem):
    core = place_ref[0]
    fetch = pltpu.make_async_copy(w_ref, wbuf, sem)
    fetch.start()
    half = REGS // 2

    def first(lo_ref, hi_ref):
        acc = jnp.zeros((8, 128), F32)
        for r in range(REGS):
            x = (lo_ref if r < half else hi_ref)[pl.ds((r % half) * 8, 8), :]
            v[pl.ds(r * 8, 8), :] = x
            acc = acc + x * x
        lam[pl.ds(0, 8), :] = acc

    @pl.when(core == 0)
    def _():
        first(mine_ref, other_ref)

    @pl.when(core != 0)
    def _():
        first(other_ref, mine_ref)

    norm0 = total(lam[pl.ds(0, 8), :])
    lane = lanes((8, 128))

    def product(k, carry):
        norm, before, table = carry
        base = pl.multiple_of(k * ROWS, 8)
        prev = pl.multiple_of(jnp.maximum(k - 1, 0) * ROWS, 8)
        for r in range(REGS):
            xs[pl.ds(r * 8, 8), :] = v[pl.ds(base + r * 8, 8), :]
        for t in range(STEPS - 1):
            tangent_step(xs, t * REGS, xs, (t + 1) * REGS, coef_ref)

        @pl.when(k == 0)
        def _():
            fetch.wait()

        last = (STEPS - 1) * REGS
        for r in range(REGS):
            lam[pl.ds(r * 8, 8), :] = (
                wbuf[pl.ds((last + r) * 8, 8), :] * xs[pl.ds((last + r) * 8, 8), :]
            )
        for t in range(STEPS - 2, -1, -1):
            adjoint_step(
                lam,
                coef_ref,
                lambda i, j, t=t: reg(wbuf, t * REGS, i, j) * reg(xs, t * REGS, i, j),
            )
        dot = jnp.zeros((8, 128), F32)
        for r in range(REGS):
            x = xs[pl.ds(r * 8, 8), :]
            image = x + lam[pl.ds(r * 8, 8), :]
            lam[pl.ds(r * 8, 8), :] = image
            dot = dot + x * image
        a = ratio(total(dot), norm)
        b = jnp.where(k > 0, ratio(norm, before), 0.0)
        new = jnp.zeros((8, 128), F32)
        for r in range(REGS):
            x = (
                lam[pl.ds(r * 8, 8), :]
                - a * xs[pl.ds(r * 8, 8), :]
                - b * v[pl.ds(prev + r * 8, 8), :]
            )
            v[pl.ds(base + ROWS + r * 8, 8), :] = x
            new = new + x * x
        table = jnp.where(lane == k, norm, table)
        table = jnp.where(lane == k + 4, a, table)
        return total(new), norm, table

    _, _, table = lax.fori_loop(
        0, ITERS, product, (norm0, jnp.ones((1, 1), F32), jnp.zeros((8, 128), F32))
    )
    for f in range(2):
        src = pl.multiple_of((core * 2 + f) * ROWS, 8)
        for i in range(NI):
            for j in range(NJ):
                start = (i // 6) * 8 * BACK + 18 * f + 6 * j + i % 6
                out_ref[pl.ds(start, 8, stride=BACK), :] = v[pl.ds(src + (i * NJ + j) * 8, 8), :]
    for g in range(4):
        out_ref[pl.ds(8 * BACK * g + 36, 8, stride=BACK), :] = table


def krylov(place, mine, other, coef, w):
    return pl.pallas_call(
        krylov_kernel,
        name="krylov",
        out_shape=jax.ShapeDtypeStruct((32 * BACK, 128), F32),
        in_specs=[SMEM, VMEM, VMEM, VMEM, ANY],
        out_specs=VMEM,
        scratch_shapes=[
            pltpu.VMEM((4 * ROWS, 128), F32),
            pltpu.VMEM((STEPS * ROWS, 128), F32),
            pltpu.VMEM((ROWS, 128), F32),
            pltpu.VMEM((STEPS * ROWS, 128), F32),
            pltpu.SemaphoreType.DMA,
        ],
        compiler_params=params(24),
        cost_estimate=cost(12),
    )(place, mine, other, coef, w)


def small_cg(norms, diag):
    n = len(norms)
    zero = jnp.zeros_like(norms[0])
    off = [ratio(norms[k], norms[k - 1]) for k in range(1, n)]

    def image(p):
        q = []
        for k in range(n + 1):
            s = zero
            if k >= 1:
                s = s + p[k - 1]
            if k < n:
                s = s + diag[k] * p[k]
            if k + 1 < n:
                s = s + off[k] * p[k + 1]
            q.append(s)
        return q

    def dot(p, q):
        s = zero
        for k in range(n):
            s = s + norms[k] * p[k] * q[k]
        return jnp.sum(s, axis=0, keepdims=True)

    residual = [zero + 1.0] + [zero] * n
    direction = list(residual)
    control = [zero] * n
    rr = dot(residual, residual)
    for it in range(ITERS):
        h = image(direction)
        step = rr / dot(direction, h)
        control = [c + step * d for c, d in zip(control, direction)]
        residual = [r - step * x for r, x in zip(residual, h)]
        if it + 1 < ITERS:
            new = dot(residual, residual)
            direction = [r + new / rr * d for r, d in zip(residual, direction)]
            rr = new
    return control, residual


def finish_kernel(place_ref, own_ref, other_ref, inc_ref, res_ref, tab, wide):
    core = place_ref[0]
    block = place_ref[1]
    table = own_ref[pl.ds(36, 32, stride=BACK), :]
    control, residual = small_cg(
        [table[:, k : k + 1] for k in range(ITERS)],
        [table[:, 4 + k : 5 + k] for k in range(ITERS)],
    )
    lane = lanes((32, 128))
    packed = jnp.zeros((32, 128), F32)
    for k, x in enumerate(control + residual):
        packed = jnp.where(lane == k, x, packed)
    tab[...] = packed
    mine = tab[pl.ds(pl.multiple_of(block * 8, 8), 8), :]
    coef = [jnp.broadcast_to(mine[:, k : k + 1], (8, 128)) for k in range(7)]
    here = block * 8 * BACK

    def fields(i, j):
        out = []
        for k in range(4):
            row = 18 * (k % 2) + 6 * j + i
            a = own_ref[pl.ds(here + row, 8, stride=BACK), :]
            b = other_ref[pl.ds(row, 8, stride=BACK), :]
            out.append(jnp.where(core == k // 2, a, b))
        return out

    for i in range(6):
        inc, res = [], []
        for j in range(NJ):
            v = fields(i, j)
            inc.append(coef[0] * v[0] + coef[1] * v[1] + coef[2] * v[2])
            res.append(coef[3] * v[0] + coef[4] * v[1] + coef[5] * v[2] + coef[6] * v[3])
        for b in range(3):
            res_ref[i, :, 128 * b : 128 * b + 128] = to_natural(res, b, 1)
        for b in range(12):
            x = to_natural(inc, b, 4)
            for e in range(4):
                wide[b, pl.ds(4 * i + e, 8, stride=24), :] = x
    for b in range(12):
        inc_ref[:, 128 * b : 128 * b + 128] = wide[b]


def finish(place, own, other):
    return pl.pallas_call(
        finish_kernel,
        name="finish",
        out_shape=(
            jax.ShapeDtypeStruct((192, 1536), F32),
            jax.ShapeDtypeStruct((6, 8, 384), F32),
        ),
        in_specs=[SMEM, VMEM, VMEM],
        out_specs=(VMEM, VMEM),
        scratch_shapes=[pltpu.VMEM((32, 128), F32), pltpu.VMEM((12, 192, 128), F32)],
        compiler_params=params(16),
        cost_estimate=cost(3),
    )(place, own, other.reshape(-1, 128))


def on_device(innovations, obs_counts, diffusion, courant):
    core = lax.axis_index("tm_1")
    block = lax.axis_index(TM)
    place = jnp.stack([core, block, lax.axis_index("space_2")]).astype(jnp.int32)
    turn = lambda x: lax.all_to_all(x.reshape(32, -1, 128), TURN, 0, 0, tiled=True)
    rows = lambda x: x.reshape(-1, 128)

    w = held(obs_counts)
    cross, w = lax.optimization_barrier((crossed(w), w))
    chunks = scatter(
        place,
        w,
        jnp.transpose(diffusion, (1, 0, 2)),
        jnp.transpose(courant, (1, 0, 2)),
        innovations.reshape(3, 768, 1536),
    )
    line, chunks = lax.optimization_barrier((lined(cross), chunks))
    own = turn(chunks)
    behind, ahead = shift(line, "space_2", 1), shift(line, "space_2", -1)
    field = own[:, :FIELD]
    other = swap(field, "tm_1")
    keep, send, coef = rhs_part(place, rows(own), other)
    part = keep + swap(send, "tm_1")
    near = swap(part, "tm_0")
    far = (shift(behind[0], "space_2", 1), shift(ahead[1], "space_2", -1))
    pieces = [rows(x) for x in (line, ahead, jnp.stack(far), behind)]
    w = weights(place, pieces + [swap(x, "tm_1") for x in pieces])
    mine = part + near
    out = turn(krylov(place, mine, swap(mine, "tm_1"), coef, w))
    theirs = swap(lax.dynamic_slice_in_dim(out, (block + 1 - 2 * core) * 8, 8, 0), "tm_1")
    increment, residual = finish(place, out.reshape(-1, 128), theirs)
    return (increment.reshape(8, 24, 1536), jnp.transpose(residual, (1, 0, 2)))


def solution(mesh):
    torus = Mesh(
        mesh.devices.reshape(2, 4, 4, 2, 2), ("space_0", "space_1", "space_2", "tm_0", "tm_1")
    )
    return jax.shard_map(
        on_device,
        mesh=torus,
        in_specs=(
            P(TM, None, SPACE, None),
            P(TM, SPACE, None),
            P(None, SPACE, None),
            P(None, SPACE, None),
        ),
        out_specs=(P(TM, SPACE, None), P(TM, SPACE, None)),
        check_vma=False,
    )
```

```python
import functools

import jax
import jax.numpy as jnp
from jax import lax
from jax.experimental import pallas as pl
from jax.experimental.pallas import tpu as pltpu
from jax.sharding import Mesh
from jax.sharding import PartitionSpec as P

SPACE = ("space_0", "space_1", "space_2")
TURN = ("space_2", "space_0", "space_1")
TM = ("tm_0", "tm_1")
SWAP = [(0, 1), (1, 0)]
F32 = jnp.float32
BF16 = jnp.bfloat16

NI, NJ = 24, 3
REGS = NI * NJ
ROWS = REGS * 8
STEPS = 12
ITERS = 3
AT_F, WIDTH = 18, 72
PIECE = 56
FIELD = 24
BACK = 40
VMEM = pl.BlockSpec(memory_space=pltpu.VMEM)
ANY = pl.BlockSpec(memory_space=pl.ANY)


def params(mib):
    return pltpu.CompilerParams(vmem_limit_bytes=mib * 2**20)


def cost(us):
    return pl.CostEstimate(flops=int(us * 10**7), bytes_accessed=10**6, transcendentals=0)


def section():
    core = lax.axis_index("tm_1")
    return core, 2 * lax.axis_index("tm_0") + core


def lanes(shape):
    return lax.broadcasted_iota(jnp.int32, shape, 1)


def pick(index, blocks, which):
    out = None
    for k, x in enumerate(blocks):
        y = jnp.take_along_axis(x, index, axis=1, mode="promise_in_bounds")
        out = y if out is None else jnp.where(which == k, y, out)
    return out


def to_held(blocks):
    shape = blocks[0].shape
    out = []
    for j in range(NJ):
        column = lanes(shape) * NJ + j
        out.append(pick(column & 127, blocks, column >> 7))
    return out


def to_natural(held, b, repeat):
    shape = held[0].shape
    column = (lanes(shape) + 128 * b) // repeat
    lane = (column * 43691) >> 17
    return pick(lane, held, column - lane * NJ)


def held_kernel(counts_ref, out_ref):
    for t in range(3):
        w = to_held([counts_ref[t, :, 128 * b : 128 * b + 128].astype(F32) for b in range(3)])
        for j in range(NJ):
            for k in range(16):
                out_ref[pl.ds(PIECE * k + 18 * t + 6 * j, 6), :] = w[j]
    for k in range(16):
        out_ref[pl.ds(PIECE * k + 54, 2), :] = jnp.zeros((2, 128), F32)


def held(counts):
    return pl.pallas_call(
        held_kernel,
        name="held",
        out_shape=jax.ShapeDtypeStruct((16 * PIECE, 128), F32),
        in_specs=[VMEM],
        out_specs=VMEM,
        compiler_params=params(4),
        cost_estimate=cost(0.5),
    )(counts)


def scatter_kernel(
    w_ref, diff_ref, cour_ref, fine_ref, out_ref, mean_ref, sums_ref
):
    @pl.when(pl.program_id(0) == 0)
    def _():
        shape = (512, 128)
        row = lax.broadcasted_iota(jnp.int32, shape, 0)
        mean_ref[...] = jnp.where((row >> 2) == lanes(shape), 1.0 / 16.0, 0.0).astype(BF16)

    def store(row, value):
        out_ref[pl.ds(row, 8, stride=WIDTH), :] = value

    core = section()[0]
    for i in range(6):
        blocks = [
            jnp.where(
                core == 0,
                diff_ref[i, :, 128 * b : 128 * b + 128],
                cour_ref[i, :, 128 * b : 128 * b + 128],
            )
            for b in range(3)
        ]
        for j, x in enumerate(to_held(blocks)):
            store(6 * j + i, x)
    for t in range(3):
        for b in range(3):
            sums_ref[3 * t + b] = jnp.dot(
                fine_ref[t, :, 512 * b : 512 * b + 512],
                mean_ref[...],
                preferred_element_type=F32,
            )
        for i in range(6):
            blocks = [
                (
                    sums_ref[3 * t + b, pl.ds(4 * i, 8, stride=24), :]
                    + sums_ref[3 * t + b, pl.ds(4 * i + 1, 8, stride=24), :]
                )
                + (
                    sums_ref[3 * t + b, pl.ds(4 * i + 2, 8, stride=24), :]
                    + sums_ref[3 * t + b, pl.ds(4 * i + 3, 8, stride=24), :]
                )
                for b in range(3)
            ]
            for j, x in enumerate(to_held(blocks)):
                row = 18 * t + 6 * j + i
                w = jnp.broadcast_to(w_ref[pl.ds(row, 1), :], (8, 128))
                store(AT_F + row, w * x)


def scatter(w, diffusion, courant, fine):
    return pl.pallas_call(
        scatter_kernel,
        name="scatter",
        grid=(4,),
        out_shape=jax.ShapeDtypeStruct((32 * WIDTH, 128), F32),
        in_specs=[
            pl.BlockSpec((PIECE, 128), lambda g: (0, 0)),
            pl.BlockSpec((6, 8, 384), lambda g: (0, g, 0)),
            pl.BlockSpec((6, 8, 384), lambda g: (0, g, 0)),
            pl.BlockSpec((3, 192, 1536), lambda g: (0, g, 0)),
        ],
        out_specs=pl.BlockSpec((8 * WIDTH, 128), lambda g: (g, 0)),
        scratch_shapes=[
            pltpu.VMEM((512, 128), BF16),
            pltpu.VMEM((9, 192, 128), F32),
        ],
        compiler_params=params(57),
        cost_estimate=cost(8),
    )(w, diffusion, courant, fine)


def reg(ref, base, i, j):
    return ref[pl.ds((base + i * NJ + j) * 8, 8), :]


def put(ref, base, i, j, value):
    ref[pl.ds((base + i * NJ + j) * 8, 8), :] = value


def taken(ref, width, first, i, j):
    return ref[pl.ds((i // 6) * 8 * width + first + 6 * j + i % 6, 8, stride=width), :]


def edges():
    sub = lax.broadcasted_iota(jnp.int32, (8, 128), 0)
    first, last = sub == 0, sub == 7
    north = lambda x: jnp.where(first, 0.0, pltpu.roll(x, 1, 0))
    south = lambda x: jnp.where(last, 0.0, pltpu.roll(x, 7, 0))
    return north, south


def west(row, j):
    return row[j - 1] if j else pltpu.roll(row[NJ - 1], 1, 1)


def east(row, j):
    return row[j + 1] if j + 1 < NJ else pltpu.roll(row[0], 127, 1)


def tangent_step(src, sb, dst, db, coef):
    north, south = edges()
    load = lambda i: [reg(src, sb, i, j) for j in range(NJ)]
    first, last = load(0), load(NI - 1)
    above = [north(x) for x in last]
    here = first
    for i in range(NI):
        below = load(i + 1) if i + 1 < NI else [south(x) for x in first]
        for j in range(NJ):
            put(
                dst,
                db,
                i,
                j,
                reg(coef, 0, i, j) * here[j]
                + reg(coef, REGS, i, j) * (above[j] + below[j] + east(here, j))
                + reg(coef, 2 * REGS, i, j) * west(here, j),
            )
        above, here = here, below


def adjoint_step(lam, coef, term):
    north, south = edges()

    def load(i):
        y = [reg(lam, 0, i, j) for j in range(NJ)]
        return y, [reg(coef, REGS, i, j) * y[j] for j in range(NJ)]

    above = [north(z) for z in load(NI - 1)[1]]
    y, here = load(0)
    wrap = [south(z) for z in here]
    for i in range(NI):
        y_next, below = load(i + 1) if i + 1 < NI else (None, wrap)
        both = [reg(coef, 2 * REGS, i, j) * y[j] for j in range(NJ)]
        new = [
            reg(coef, 0, i, j) * y[j] + (above[j] + below[j]) + (west(here, j) + east(both, j))
            for j in range(NJ)
        ]
        for j in range(NJ):
            add = term(i, j)
            put(lam, 0, i, j, new[j] if add is None else new[j] + add)
        above, here, y = here, below, y_next


def rhs_kernel(own_ref, other_ref, keep_ref, send_ref, coef_ref, lam):
    core, block = section()

    def coefficients(diff_ref, diff_width, cour_ref, cour_width):
        for i in range(NI):
            for j in range(NJ):
                d = taken(diff_ref, diff_width, 0, i, j)
                c = taken(cour_ref, cour_width, 0, i, j)
                put(coef_ref, 0, i, j, 1.0 - 4.0 * d - c)
                put(coef_ref, REGS, i, j, d)
                put(coef_ref, 2 * REGS, i, j, d + c)

    @pl.when(core == 0)
    def _():
        coefficients(own_ref, WIDTH, other_ref, FIELD)

    @pl.when(core != 0)
    def _():
        coefficients(other_ref, FIELD, own_ref, WIDTH)

    for i in range(NI):
        for j in range(NJ):
            put(lam, 0, i, j, taken(own_ref, WIDTH, AT_F + 36, i, j))
    for t in (1, 0):
        adjoint_step(lam, coef_ref, lambda i, j, t=t: taken(own_ref, WIDTH, AT_F + 18 * t, i, j))

    def more(_, carry):
        adjoint_step(lam, coef_ref, lambda i, j: None)
        return carry

    lax.fori_loop(0, 3 * block, more, 0)
    half = ROWS // 2
    keep_ref[...] = lam[pl.ds(pl.multiple_of(core * half, 8), half), :]
    send_ref[...] = lam[pl.ds(pl.multiple_of((1 - core) * half, 8), half), :]


def rhs_part(own, other):
    return pl.pallas_call(
        rhs_kernel,
        name="rhs_part",
        out_shape=(
            jax.ShapeDtypeStruct((ROWS // 2, 128), F32),
            jax.ShapeDtypeStruct((ROWS // 2, 128), F32),
            jax.ShapeDtypeStruct((3 * ROWS, 128), F32),
        ),
        in_specs=[VMEM, VMEM],
        out_specs=(VMEM, VMEM, VMEM),
        scratch_shapes=[pltpu.VMEM((ROWS, 128), F32)],
        compiler_params=params(16),
        cost_estimate=cost(4),
    )(own, other.reshape(-1, 128))


def weights_kernel(ahead, *refs):
    out_ref = refs[-1]
    core, row = section()[0], lax.axis_index("space_2")
    for flip in range(2):
        for n, d in enumerate(ahead):
            ref = refs[len(ahead) * flip + n]
            first = jnp.bitwise_and(row + d, 3) * 6 * NJ
            for half in range(2):
                base = (jnp.bitwise_xor(core, flip) + 2 * half) * 3 * REGS + first
                for t in range(3):
                    for i in range(6):
                        for j in range(NJ):
                            at = pl.multiple_of((base + t * REGS + i * NJ + j) * 8, 8)
                            start = PIECE * half + 18 * t + 6 * j + i
                            out_ref[pl.ds(at, 8), :] = ref[pl.ds(start, 8, stride=2 * PIECE), :]


def weights(ahead, pieces, into=None):
    pieces = pieces + [swap(x, "tm_1") for x in pieces]
    more = [] if into is None else [into]
    return pl.pallas_call(
        functools.partial(weights_kernel, ahead),
        out_shape=jax.ShapeDtypeStruct((STEPS * ROWS, 128), F32),
        in_specs=[VMEM] * len(pieces + more),
        out_specs=VMEM,
        input_output_aliases={len(pieces): 0} if more else {},
        compiler_params=params(16),
        cost_estimate=cost(1 + len(ahead)),
    )(*pieces, *more)


def shift(x, axis, by):
    return lax.ppermute(x, axis, [(k, (k + by) % 4) for k in range(4)])


def swap(x, axis):
    return lax.ppermute(x, axis, SWAP)


def total(x):
    return jnp.sum(jnp.sum(x, axis=0, keepdims=True), axis=1, keepdims=True)


def ratio(a, b):
    return jnp.where(b > 0.0, a / jnp.where(b > 0.0, b, 1.0), 0.0)


def krylov_kernel(mine_ref, other_ref, coef_ref, wbuf, out_ref, v, xs, lam):
    core = section()[0]
    half = REGS // 2

    def first(lo_ref, hi_ref):
        acc = jnp.zeros((8, 128), F32)
        for r in range(REGS):
            x = (lo_ref if r < half else hi_ref)[pl.ds((r % half) * 8, 8), :]
            v[pl.ds(r * 8, 8), :] = x
            acc = acc + x * x
        lam[pl.ds(0, 8), :] = acc

    @pl.when(core == 0)
    def _():
        first(mine_ref, other_ref)

    @pl.when(core != 0)
    def _():
        first(other_ref, mine_ref)

    norm0 = total(lam[pl.ds(0, 8), :])
    lane = lanes((8, 128))

    def product(k, carry):
        norm, before, table = carry
        base = pl.multiple_of(k * ROWS, 8)
        prev = pl.multiple_of(jnp.maximum(k - 1, 0) * ROWS, 8)
        for r in range(REGS):
            xs[pl.ds(r * 8, 8), :] = v[pl.ds(base + r * 8, 8), :]
        for t in range(STEPS - 1):
            tangent_step(xs, t * REGS, xs, (t + 1) * REGS, coef_ref)

        last = (STEPS - 1) * REGS
        for r in range(REGS):
            lam[pl.ds(r * 8, 8), :] = (
                wbuf[pl.ds((last + r) * 8, 8), :] * xs[pl.ds((last + r) * 8, 8), :]
            )
        for t in range(STEPS - 2, -1, -1):
            adjoint_step(
                lam,
                coef_ref,
                lambda i, j, t=t: reg(wbuf, t * REGS, i, j) * reg(xs, t * REGS, i, j),
            )
        dot = jnp.zeros((8, 128), F32)
        for r in range(REGS):
            x = xs[pl.ds(r * 8, 8), :]
            image = x + lam[pl.ds(r * 8, 8), :]
            lam[pl.ds(r * 8, 8), :] = image
            dot = dot + x * image
        a = ratio(total(dot), norm)
        b = jnp.where(k > 0, ratio(norm, before), 0.0)
        new = jnp.zeros((8, 128), F32)
        for r in range(REGS):
            x = (
                lam[pl.ds(r * 8, 8), :]
                - a * xs[pl.ds(r * 8, 8), :]
                - b * v[pl.ds(prev + r * 8, 8), :]
            )
            v[pl.ds(base + ROWS + r * 8, 8), :] = x
            new = new + x * x
        table = jnp.where(lane == k, norm, table)
        table = jnp.where(lane == k + 4, a, table)
        return total(new), norm, table

    _, _, table = lax.fori_loop(
        0, ITERS, product, (norm0, jnp.ones((1, 1), F32), jnp.zeros((8, 128), F32))
    )
    for f in range(2):
        src = pl.multiple_of((core * 2 + f) * ROWS, 8)
        for i in range(NI):
            for j in range(NJ):
                start = (i // 6) * 8 * BACK + 18 * f + 6 * j + i % 6
                out_ref[pl.ds(start, 8, stride=BACK), :] = v[pl.ds(src + (i * NJ + j) * 8, 8), :]
    for g in range(4):
        out_ref[pl.ds(8 * BACK * g + 36, 8, stride=BACK), :] = table


def krylov(mine, other, coef, w):
    return pl.pallas_call(
        krylov_kernel,
        name="krylov",
        out_shape=jax.ShapeDtypeStruct((32 * BACK, 128), F32),
        in_specs=[VMEM] * 4,
        out_specs=VMEM,
        scratch_shapes=[
            pltpu.VMEM((4 * ROWS, 128), F32),
            pltpu.VMEM((STEPS * ROWS, 128), F32),
            pltpu.VMEM((ROWS, 128), F32),
        ],
        compiler_params=pltpu.CompilerParams(vmem_limit_bytes=16 * 2**20),
        cost_estimate=cost(12),
    )(mine, other, coef, w)


def small_cg(norms, diag):
    n = len(norms)
    zero = jnp.zeros_like(norms[0])
    off = [ratio(norms[k], norms[k - 1]) for k in range(1, n)]

    def image(p):
        q = []
        for k in range(n + 1):
            s = zero
            if k >= 1:
                s = s + p[k - 1]
            if k < n:
                s = s + diag[k] * p[k]
            if k + 1 < n:
                s = s + off[k] * p[k + 1]
            q.append(s)
        return q

    def dot(p, q):
        s = zero
        for k in range(n):
            s = s + norms[k] * p[k] * q[k]
        return jnp.sum(s, axis=0, keepdims=True)

    residual = [zero + 1.0] + [zero] * n
    direction = list(residual)
    control = [zero] * n
    rr = dot(residual, residual)
    for it in range(ITERS):
        h = image(direction)
        step = rr / dot(direction, h)
        control = [c + step * d for c, d in zip(control, direction)]
        residual = [r - step * x for r, x in zip(residual, h)]
        if it + 1 < ITERS:
            new = dot(residual, residual)
            direction = [r + new / rr * d for r, d in zip(residual, direction)]
            rr = new
    return control, residual


def finish_kernel(own_ref, other_ref, inc_ref, res_ref, tab, wide):
    core, block = section()
    table = own_ref[pl.ds(36, 32, stride=BACK), :]
    control, residual = small_cg(
        [table[:, k : k + 1] for k in range(ITERS)],
        [table[:, 4 + k : 5 + k] for k in range(ITERS)],
    )
    lane = lanes((32, 128))
    packed = jnp.zeros((32, 128), F32)
    for k, x in enumerate(control + residual):
        packed = jnp.where(lane == k, x, packed)
    tab[...] = packed
    mine = tab[pl.ds(pl.multiple_of(block * 8, 8), 8), :]
    coef = [jnp.broadcast_to(mine[:, k : k + 1], (8, 128)) for k in range(7)]
    here = block * 8 * BACK

    def fields(i, j):
        out = []
        for k in range(4):
            row = 18 * (k % 2) + 6 * j + i
            a = own_ref[pl.ds(here + row, 8, stride=BACK), :]
            b = other_ref[pl.ds(row, 8, stride=BACK), :]
            out.append(jnp.where(core == k // 2, a, b))
        return out

    for i in range(6):
        inc, res = [], []
        for j in range(NJ):
            v = fields(i, j)
            inc.append(coef[0] * v[0] + coef[1] * v[1] + coef[2] * v[2])
            res.append(coef[3] * v[0] + coef[4] * v[1] + coef[5] * v[2] + coef[6] * v[3])
        for b in range(3):
            res_ref[i, :, 128 * b : 128 * b + 128] = to_natural(res, b, 1)
        for b in range(12):
            x = to_natural(inc, b, 4)
            for e in range(4):
                wide[b, pl.ds(4 * i + e, 8, stride=24), :] = x
    for b in range(12):
        inc_ref[:, 128 * b : 128 * b + 128] = wide[b]


def finish(own, other):
    return pl.pallas_call(
        finish_kernel,
        name="finish",
        out_shape=(
            jax.ShapeDtypeStruct((192, 1536), F32),
            jax.ShapeDtypeStruct((6, 8, 384), F32),
        ),
        in_specs=[VMEM, VMEM],
        out_specs=(VMEM, VMEM),
        scratch_shapes=[pltpu.VMEM((32, 128), F32), pltpu.VMEM((12, 192, 128), F32)],
        compiler_params=params(16),
        cost_estimate=cost(3),
    )(own, other.reshape(-1, 128))


def on_device(innovations, obs_counts, diffusion, courant):
    core, block = section()
    turn = lambda x: lax.all_to_all(x.reshape(32, -1, 128), TURN, 0, 0, tiled=True)
    rows = lambda x: x.reshape(-1, 128)

    w = held(obs_counts)
    chunks = scatter(
        w,
        jnp.transpose(diffusion, (1, 0, 2)),
        jnp.transpose(courant, (1, 0, 2)),
        innovations.reshape(3, 768, 1536),
    )
    line = lax.all_to_all(
        w.reshape(16, PIECE, 128), ("space_0", "space_1", "tm_0"), 0, 0, tiled=True
    ).reshape(2, -1, 128)
    line, chunks = lax.optimization_barrier((line, chunks))
    own = turn(chunks)
    behind0, ahead1 = shift(line[0], "space_2", 1), shift(line[1], "space_2", -1)
    behind1, ahead0 = shift(line[1], "space_2", 1), shift(line[0], "space_2", -1)
    field = own[:, :FIELD]
    other = swap(field, "tm_1")
    keep, send, coef = rhs_part(rows(own), other)
    behind0, ahead1, _ = lax.optimization_barrier((behind0, ahead1, keep))
    sent = swap(send, "tm_1")
    part = keep + sent
    near = swap(part, "tm_0")
    far = (shift(behind0, "space_2", 1), shift(ahead1, "space_2", -1))
    ahead, behind = jnp.concatenate([ahead0, ahead1]), jnp.concatenate([behind0, behind1])
    w = weights((0, 1, 3), [rows(line), ahead, behind])
    w = weights((2,), [jnp.concatenate(far)], w)
    mine = part + near
    out = turn(krylov(mine, swap(mine, "tm_1"), coef, w))
    theirs = swap(lax.dynamic_slice_in_dim(out, (block + 1 - 2 * core) * 8, 8, 0), "tm_1")
    increment, residual = finish(out.reshape(-1, 128), theirs)
    return (increment.reshape(8, 24, 1536), jnp.transpose(residual, (1, 0, 2)))


def solution(mesh):
    torus = Mesh(
        mesh.devices.reshape(2, 4, 4, 2, 2), ("space_0", "space_1", "space_2", "tm_0", "tm_1")
    )
    return jax.shard_map(
        on_device,
        mesh=torus,
        in_specs=(
            P(TM, None, SPACE, None),
            P(TM, SPACE, None),
            P(None, SPACE, None),
            P(None, SPACE, None),
        ),
        out_specs=(P(TM, SPACE, None), P(TM, SPACE, None)),
        check_vma=False,
    )
```
